8 devices in a mesh: dp: 2 (over z, y), tp: 4 (over x, core).
Axes of the slice: x: 2, y: 2, z: 1, core: 2. Of those that a mesh axis runs over, the one named last changes fastest.
Arguments:
- tokens: int32 [2, 2048], P('dp'), parts along dimension 0
- doc_ids: int32 [2, 2048], P('dp'), parts along dimension 0
- embedding: bfloat16 [32000, 2048], P('tp')
- attn_norm: bfloat16 [2048], replicated
- w_q: bfloat16 [2048, 32, 64], P(None, 'tp')
- w_k: bfloat16 [2048, 4, 64], P(None, 'tp')
- w_v: bfloat16 [2048, 4, 64], P(None, 'tp')
- w_o: bfloat16 [32, 64, 2048], P('tp')
- mlp_norm: bfloat16 [2048], replicated
- w_gate: bfloat16 [2048, 5632], P(None, 'tp')
- w_up: bfloat16 [2048, 5632], P(None, 'tp')
- w_down: bfloat16 [5632, 2048], P('tp')
- d_out: bfloat16 [2, 2048, 2048], P('dp', 'tp'), parts along dimension 0
Outputs:
- output 1: bfloat16 [2, 2048, 2048], P('dp', 'tp'), parts along dimension 0
- output 2: float32 [64000, 2048], P(('dp', 'tp')), parts along dimension 0
- output 3: float32 [4096], P('dp'), parts along dimension 0
- output 4: float32 [4096, 32, 64], P('dp', 'tp'), parts along dimension 0
- output 5: float32 [4096, 4, 64], P('dp', 'tp'), parts along dimension 0
- output 6: float32 [4096, 4, 64], P('dp', 'tp'), parts along dimension 0
- output 7: float32 [64, 64, 2048], P(('dp', 'tp')), parts along dimension 0
- output 8: float32 [4096], P('dp'), parts along dimension 0
- output 9: float32 [4096, 5632], P('dp', 'tp'), parts along dimension 0
- output 10: float32 [4096, 5632], P('dp', 'tp'), parts along dimension 0
- output 11: float32 [11264, 2048], P(('dp', 'tp')), parts along dimension 0
There are 2 independent parts. The reference program is written for one: setup_inputs(seed, part) draws one part's arguments, and reference() takes and returns one part's arrays. A program takes and returns all parts, laid end to end along the dimension named above; an argument that names none is the same for every part.
All inputs are finite; a program needn't handle non-finite values.
Results may differ from the reference program's by a relative error of at most 0.02.
Values are sent between devices in bfloat16 or wider.
A program may use at most 1 GiB of HBM per device.

```python
import math
import jax
import jax.numpy as jnp
from jax import lax

N_ROWS = 1
SEQ_LEN = 2048
VOCAB_SIZE = 32000
MODEL_DIM = 2048
NUM_HEADS = 32
KV_HEADS = 4
HEAD_DIM = 64
FFN_DIM = 5632

NORM_EPS = 1e-5
ROPE_THETA = 500000.0
GROUP_SIZE = NUM_HEADS // KV_HEADS


def setup_inputs(seed: int = 0, part: int = 0) -> dict:
    part_keys = jax.random.split(jax.random.fold_in(jax.random.key(seed), part), 6)
    shared_keys = jax.random.split(jax.random.key(seed + 1), 10)
    low_span = max(VOCAB_SIZE // 16, 1)
    doc_span = max(SEQ_LEN // 4, 1)
    chooser = jax.random.randint(part_keys[0], (N_ROWS, SEQ_LEN), 0, 2)
    any_ids = jax.random.randint(part_keys[1], (N_ROWS, SEQ_LEN), 0, VOCAB_SIZE)
    low_ids = jax.random.randint(part_keys[2], (N_ROWS, SEQ_LEN), 0, low_span)
    tokens = jnp.where(chooser == 0, any_ids, low_ids).astype(jnp.int32)
    starts = (jax.random.randint(part_keys[3], (N_ROWS, SEQ_LEN), 0, doc_span) == 0).astype(jnp.int32)
    doc_ids = jnp.cumsum(starts, axis=1).astype(jnp.int32)
    attn_dim = NUM_HEADS * HEAD_DIM

    def draw_normal(key_index, arr_shape, factor):
        return (jax.random.normal(shared_keys[key_index], arr_shape, jnp.float32) * factor).astype(jnp.bfloat16)

    return {
        "tokens": tokens,
        "doc_ids": doc_ids,
        "embedding": draw_normal(0, (VOCAB_SIZE, MODEL_DIM), 1.0),
        "attn_norm": (1.0 + 0.3 * jax.random.normal(shared_keys[1], (MODEL_DIM,), jnp.float32)).astype(jnp.bfloat16),
        "w_q": draw_normal(2, (MODEL_DIM, NUM_HEADS, HEAD_DIM), MODEL_DIM ** -0.5),
        "w_k": draw_normal(3, (MODEL_DIM, KV_HEADS, HEAD_DIM), MODEL_DIM ** -0.5),
        "w_v": draw_normal(4, (MODEL_DIM, KV_HEADS, HEAD_DIM), 2.0 * MODEL_DIM ** -0.5),
        "w_o": draw_normal(5, (NUM_HEADS, HEAD_DIM, MODEL_DIM), 2.0 * attn_dim ** -0.5),
        "mlp_norm": (1.0 + 0.3 * jax.random.normal(shared_keys[6], (MODEL_DIM,), jnp.float32)).astype(jnp.bfloat16),
        "w_gate": draw_normal(7, (MODEL_DIM, FFN_DIM), MODEL_DIM ** -0.5),
        "w_up": draw_normal(8, (MODEL_DIM, FFN_DIM), MODEL_DIM ** -0.5),
        "w_down": draw_normal(9, (FFN_DIM, MODEL_DIM), 1.5 * FFN_DIM ** -0.5),
        "d_out": jax.random.normal(part_keys[4], (N_ROWS, SEQ_LEN, MODEL_DIM), jnp.float32).astype(jnp.bfloat16),
    }


def rope_tables():
    half_dim = HEAD_DIM // 2
    inv_freq = 1.0 / (ROPE_THETA ** (jnp.arange(half_dim, dtype=jnp.float32) * 2.0 / HEAD_DIM))
    wavelen = 2.0 * math.pi / inv_freq
    smooth = (8192.0 / wavelen - 1.0) / 3.0
    scaled = jnp.where(wavelen > 8192.0, inv_freq / 8.0, (1.0 - smooth) * inv_freq / 8.0 + smooth * inv_freq)
    inv_freq = jnp.where(wavelen < 2048.0, inv_freq, scaled)
    angles = jnp.arange(SEQ_LEN, dtype=jnp.float32)[:, None] * inv_freq[None, :]
    return jnp.cos(angles), jnp.sin(angles)


def as_bf16(values):
    return values.astype(jnp.bfloat16).astype(jnp.float32)


def rms_norm(values, gain_vec):
    inv_rms = lax.rsqrt(jnp.mean(values * values, axis=-1, keepdims=True) + NORM_EPS)
    return as_bf16(values * inv_rms * gain_vec)


def rotate(values, cos_t, sin_t):
    half_dim = HEAD_DIM // 2
    x_first = values[..., :half_dim]
    x_second = values[..., half_dim:]
    cos_b = cos_t[:, None, :]
    sin_b = sin_t[:, None, :]
    return jnp.concatenate([x_first * cos_b - x_second * sin_b, x_second * cos_b + x_first * sin_b], axis=-1)


def attend_group(group_items):
    q_grp, k_grp, v_grp, doc_row = group_items
    positions = jnp.arange(SEQ_LEN)
    allowed = (positions[:, None] >= positions[None, :]) & (doc_row[:, None] == doc_row[None, :])
    scores = jnp.einsum("qgd,kd->gqk", q_grp, k_grp) * HEAD_DIM ** -0.5
    scores = jnp.where(allowed[None], scores, -1e30)
    attn_probs = as_bf16(jax.nn.softmax(scores, axis=-1))
    return as_bf16(jnp.einsum("gqk,kd->qgd", attn_probs, v_grp))


def layer_forward(x_emb, doc_ids, attn_norm, w_q, w_k, w_v, w_o, mlp_norm, w_gate, w_up, w_down):
    cos_t, sin_t = rope_tables()
    n_tok = N_ROWS * SEQ_LEN
    h_one = rms_norm(x_emb, attn_norm).reshape(n_tok, MODEL_DIM)
    q_proj = as_bf16(jnp.dot(h_one, w_q.reshape(MODEL_DIM, NUM_HEADS * HEAD_DIM)))
    k_proj = as_bf16(jnp.dot(h_one, w_k.reshape(MODEL_DIM, KV_HEADS * HEAD_DIM)))
    v_proj = as_bf16(jnp.dot(h_one, w_v.reshape(MODEL_DIM, KV_HEADS * HEAD_DIM)))
    q_rot = as_bf16(rotate(q_proj.reshape(N_ROWS, SEQ_LEN, NUM_HEADS, HEAD_DIM), cos_t, sin_t))
    k_rot = as_bf16(rotate(k_proj.reshape(N_ROWS, SEQ_LEN, KV_HEADS, HEAD_DIM), cos_t, sin_t))
    v_heads = v_proj.reshape(N_ROWS, SEQ_LEN, KV_HEADS, HEAD_DIM)
    q_items = q_rot.reshape(N_ROWS, SEQ_LEN, KV_HEADS, GROUP_SIZE, HEAD_DIM).transpose(0, 2, 1, 3, 4)
    q_items = q_items.reshape(N_ROWS * KV_HEADS, SEQ_LEN, GROUP_SIZE, HEAD_DIM)
    k_items = k_rot.transpose(0, 2, 1, 3).reshape(N_ROWS * KV_HEADS, SEQ_LEN, HEAD_DIM)
    v_items = v_heads.transpose(0, 2, 1, 3).reshape(N_ROWS * KV_HEADS, SEQ_LEN, HEAD_DIM)
    doc_items = jnp.repeat(doc_ids, KV_HEADS, axis=0)
    attn_items = lax.map(jax.checkpoint(attend_group), (q_items, k_items, v_items, doc_items))
    attn_flat = attn_items.reshape(N_ROWS, KV_HEADS, SEQ_LEN, GROUP_SIZE, HEAD_DIM).transpose(0, 2, 1, 3, 4)
    attn_flat = attn_flat.reshape(n_tok, NUM_HEADS * HEAD_DIM)
    attn_res = as_bf16(jnp.dot(attn_flat, w_o.reshape(NUM_HEADS * HEAD_DIM, MODEL_DIM)))
    x_mid = as_bf16(x_emb.reshape(n_tok, MODEL_DIM) + attn_res)
    h_two = rms_norm(x_mid, mlp_norm)
    gate_proj = as_bf16(jnp.dot(h_two, w_gate))
    up_proj = as_bf16(jnp.dot(h_two, w_up))
    mid_act = as_bf16(jax.nn.silu(gate_proj) * up_proj)
    y_out = as_bf16(x_mid + as_bf16(jnp.dot(mid_act, w_down)))
    return y_out.reshape(N_ROWS, SEQ_LEN, MODEL_DIM)


def reference(tokens, doc_ids, embedding, attn_norm, w_q, w_k, w_v, w_o, mlp_norm, w_gate, w_up, w_down, d_out):
    weights = [weight.astype(jnp.float32) for weight in (embedding, attn_norm, w_q, w_k, w_v, w_o, mlp_norm, w_gate, w_up, w_down)]

    def forward(embed_f32, *layer_weights):
        x_emb = jnp.take(embed_f32, tokens, axis=0)
        return layer_forward(x_emb, doc_ids, *layer_weights)

    y_out, pullback = jax.vjp(forward, *weights)
    cotangents = pullback(d_out.astype(jnp.float32))
    return (y_out.astype(jnp.bfloat16),) + tuple(cotangents)
```

```python
import functools
import math
import jax
import jax.numpy as jnp
from jax import lax
from jax.experimental import pallas as pl
from jax.experimental.pallas import tpu as pltpu
from jax.sharding import PartitionSpec as P

NORM_EPS = 1e-5
ROPE_THETA = 500000.0
BQ = 256
BK = 256
HEADS = 8
HD = 64
HALF = HD // 2
LOG2E = 1.4426950408889634
SCALE2 = LOG2E * HD ** -0.5
NEG = -1e30
ROWS_OUT = 200
F32 = jnp.float32
BF16 = jnp.bfloat16


def rope_tables_t(positions):
    inv_freq = 1.0 / (ROPE_THETA ** (jnp.arange(HALF, dtype=F32) * 2.0 / HD))
    wavelen = 2.0 * math.pi / inv_freq
    smooth = (8192.0 / wavelen - 1.0) / 3.0
    scaled = jnp.where(wavelen > 8192.0, inv_freq / 8.0, (1.0 - smooth) * inv_freq / 8.0 + smooth * inv_freq)
    inv_freq = jnp.where(wavelen < 2048.0, inv_freq, scaled)
    angles = inv_freq[:, None] * positions.astype(F32)[None, :]
    return jnp.cos(angles), jnp.sin(angles)


def dot(a, b, ca, cb):
    return lax.dot_general(a, b, (((ca,), (cb,)), ((), ())), preferred_element_type=F32)


def rms_forward(values, gain_vec):
    values32 = values.astype(F32)
    inv_rms = lax.rsqrt(jnp.mean(values32 * values32, axis=-1, keepdims=True) + NORM_EPS)
    return (values32 * inv_rms * gain_vec.astype(F32)).astype(BF16), inv_rms


def rms_backward(d_scaled32, values, inv_rms, gain_vec):
    normed = values.astype(F32) * inv_rms
    d_gain = jnp.sum(d_scaled32 * normed, axis=0)
    d_normed = d_scaled32 * gain_vec.astype(F32)
    d_values = inv_rms * (d_normed - normed * jnp.mean(d_normed * normed, axis=-1, keepdims=True))
    return d_values, d_gain


def rel_col(block, shard_bits, block_size):
    per = 512 // block_size
    return pl.multiple_of(((block // per) ^ shard_bits) * 512 + (block % per) * block_size, block_size)


def rope_keys(kv_ref, cos_ref, sin_ref):
    k1 = kv_ref[0:HALF, :].astype(F32)
    k2 = kv_ref[HALF:HD, :].astype(F32)
    cos_v = cos_ref[...]
    sin_v = sin_ref[...]
    return jnp.concatenate([k1 * cos_v - k2 * sin_v, k2 * cos_v + k1 * sin_v], axis=0)


def key_bias(kblk, qblk, qs_row):
    kpos = kblk * BK + lax.broadcasted_iota(jnp.int32, (BK, BQ), 0)
    qpos = qblk * BQ + lax.broadcasted_iota(jnp.int32, (BK, BQ), 1)
    return jnp.where((kpos <= qpos) & (kpos >= qs_row), 0.0, NEG)


def attn_fwd_kernel(start, s_ref, q_ref, kv_ref, cos_ref, sin_ref, qs_ref, o_ref, qr_ref, lse_ref,
                    k_scr, acc, m_scr, l_scr, bias):
    i = pl.program_id(0)
    me = s_ref[8]

    @pl.when(i == 0)
    def _():
        k_scr[...] = rope_keys(kv_ref, cos_ref, sin_ref).T.astype(BF16)

    rb = start + i
    qcol = pl.multiple_of(rb * BQ, BQ)
    ab = ((rb // 2) ^ me) * 2 + rb % 2
    cos_v = cos_ref[:, pl.ds(qcol, BQ)]
    sin_v = sin_ref[:, pl.ds(qcol, BQ)]
    qs_row = qs_ref[:, pl.ds(qcol, BQ)]
    for h in range(HEADS):
        q1 = q_ref[h * HD:h * HD + HALF, :].astype(F32)
        q2 = q_ref[h * HD + HALF:(h + 1) * HD, :].astype(F32)
        qr_ref[h * HD:h * HD + HALF, :] = (q1 * cos_v - q2 * sin_v).astype(BF16)
        qr_ref[h * HD + HALF:(h + 1) * HD, :] = (q2 * cos_v + q1 * sin_v).astype(BF16)
    acc[...] = jnp.zeros_like(acc)
    m_scr[...] = jnp.full_like(m_scr, NEG)
    l_scr[...] = jnp.zeros_like(l_scr)

    def step(j, carry):
        col = rel_col(j, me, BK)
        k_blk = k_scr[pl.ds(col, BK), :]
        v_blk = kv_ref[HD:2 * HD, pl.ds(col, BK)]
        bias[...] = key_bias(j, ab, qs_row)
        for h in range(HEADS):
            rows = slice(h * HD, (h + 1) * HD)
            s = dot(k_blk, qr_ref[rows, :], 1, 0) * SCALE2 + bias[...]
            m_old = m_scr[h:h + 1, :]
            m_new = jnp.maximum(m_old, jnp.max(s, axis=0, keepdims=True))
            p = jnp.exp2(s - m_new)
            alpha = jnp.exp2(m_old - m_new)
            l_scr[h:h + 1, :] = l_scr[h:h + 1, :] * alpha + jnp.sum(p, axis=0, keepdims=True)
            m_scr[h:h + 1, :] = m_new
            acc[rows, :] = acc[rows, :] * alpha + dot(v_blk, p.astype(BF16), 1, 0)
        return carry

    lax.fori_loop(s_ref[ab], ab + 1, step, 0)
    for h in range(HEADS):
        rows = slice(h * HD, (h + 1) * HD)
        o_ref[rows, :] = (acc[rows, :] / l_scr[h:h + 1, :]).astype(BF16)
    lse_ref[...] = m_scr[...] + jnp.log2(l_scr[...])


def attn_fwd(scal, qkv_t, cos_t, sin_t, qs_row, start, count):
    width = count * BQ
    whole = lambda i, s: (0, 0)
    return pl.pallas_call(
        functools.partial(attn_fwd_kernel, start),
        grid_spec=pltpu.PrefetchScalarGridSpec(
            num_scalar_prefetch=1,
            grid=(count,),
            in_specs=[
                pl.BlockSpec((HEADS * HD, BQ), lambda i, s: (0, start + i)),
                pl.BlockSpec((2 * HD, 2048), lambda i, s: (4, 0)),
                pl.BlockSpec((HALF, 2048), whole),
                pl.BlockSpec((HALF, 2048), whole),
                pl.BlockSpec((1, 2048), whole),
            ],
            out_specs=[
                pl.BlockSpec((HEADS * HD, BQ), lambda i, s: (0, i)),
                pl.BlockSpec((HEADS * HD, BQ), lambda i, s: (0, i)),
                pl.BlockSpec((HEADS, BQ), lambda i, s: (0, i)),
            ],
            scratch_shapes=[
                pltpu.VMEM((2048, HD), BF16),
                pltpu.VMEM((HEADS * HD, BQ), F32),
                pltpu.VMEM((HEADS, BQ), F32),
                pltpu.VMEM((HEADS, BQ), F32),
                pltpu.VMEM((BK, BQ), F32),
            ],
        ),
        out_shape=[
            jax.ShapeDtypeStruct((HEADS * HD, width), BF16),
            jax.ShapeDtypeStruct((HEADS * HD, width), BF16),
            jax.ShapeDtypeStruct((HEADS, width), F32),
        ],
        compiler_params=pltpu.CompilerParams(dimension_semantics=("arbitrary",), vmem_limit_bytes=48 << 20),
        cost_estimate=pl.CostEstimate(flops=int(10e9), bytes_accessed=8 << 20, transcendentals=0),
        name="attn_fwd",
    )(scal, qkv_t, qkv_t, cos_t, sin_t, qs_row)


def attn_bwd_kernel(start, last, s_ref, qr_ref, do_ref, o_ref, lse_ref, kv_ref, cos_ref, sin_ref, qs_ref, *rest):
    if last:
        dk_in, dv_in, dq_ref, dkv_ref, dk, dv, k_scr, kt_scr, v_scr, qcat, docat, delta, dq, bias, p_scr, ds_scr = rest
    else:
        dq_ref, dk, dv, k_scr, kt_scr, v_scr, qcat, docat, delta, dq, bias, p_scr, ds_scr = rest
    i = pl.program_id(0)
    me = s_ref[8]

    @pl.when(i == 0)
    def _():
        kt = rope_keys(kv_ref, cos_ref, sin_ref)
        kt_scr[...] = kt.astype(BF16)
        k_scr[...] = kt.T.astype(BF16)
        v_scr[...] = kv_ref[HD:2 * HD, :].astype(F32).T.astype(BF16)
        if last:
            dk[...] = dk_in[...]
            dv[...] = dv_in[...]
        else:
            dk[...] = jnp.zeros_like(dk)
            dv[...] = jnp.zeros_like(dv)

    rb = start + i
    qcol = pl.multiple_of(rb * BQ, BQ)
    ab = ((rb // 2) ^ me) * 2 + rb % 2
    qs_row = qs_ref[:, pl.ds(qcol, BQ)]
    for h in range(HEADS):
        rows = slice(h * HD, (h + 1) * HD)
        cols = slice(h * BQ, (h + 1) * BQ)
        do_h = do_ref[rows, :]
        qcat[:, cols] = qr_ref[rows, :]
        docat[:, cols] = do_h
        delta[h:h + 1, :] = jnp.sum(o_ref[rows, :].astype(F32) * do_h.astype(F32), axis=0, keepdims=True)
    dq[...] = jnp.zeros_like(dq)

    def step(j, carry):
        col = rel_col(j, me, BK)
        k_blk = k_scr[pl.ds(col, BK), :]
        v_blk = v_scr[pl.ds(col, BK), :]
        bias[...] = key_bias(j, ab, qs_row)
        for h in range(HEADS):
            cols = slice(h * BQ, (h + 1) * BQ)
            s = dot(k_blk, qcat[:, cols], 1, 0) * SCALE2 + bias[...]
            p = jnp.exp2(s - lse_ref[h:h + 1, :])
            d_p = dot(v_blk, docat[:, cols], 1, 0)
            p_scr[:, cols] = p.astype(BF16)
            ds_scr[:, cols] = (p * (d_p - delta[h:h + 1, :])).astype(BF16)
        dv[pl.ds(col, BK), :] += dot(p_scr[...], docat[...], 1, 1)
        dk[pl.ds(col, BK), :] += dot(ds_scr[...], qcat[...], 1, 1)
        dq[...] += dot(kt_scr[:, pl.ds(col, BK)], ds_scr[...], 1, 0)
        return carry

    lax.fori_loop(s_ref[ab], ab + 1, step, 0)
    cos_v = cos_ref[:, pl.ds(qcol, BQ)]
    sin_v = sin_ref[:, pl.ds(qcol, BQ)]
    for h in range(HEADS):
        cols = slice(h * BQ, (h + 1) * BQ)
        g1 = dq[0:HALF, cols] * HD ** -0.5
        g2 = dq[HALF:HD, cols] * HD ** -0.5
        dq_ref[h * HD:h * HD + HALF, :] = (g1 * cos_v + g2 * sin_v).astype(BF16)
        dq_ref[h * HD + HALF:(h + 1) * HD, :] = (g2 * cos_v - g1 * sin_v).astype(BF16)

    if last:
        @pl.when(i == pl.num_programs(0) - 1)
        def _():
            kt = dk[...].T * HD ** -0.5
            g1 = kt[0:HALF, :]
            g2 = kt[HALF:HD, :]
            cos_a = cos_ref[...]
            sin_a = sin_ref[...]
            dkv_ref[0:HALF, :] = (g1 * cos_a + g2 * sin_a).astype(BF16)
            dkv_ref[HALF:HD, :] = (g2 * cos_a - g1 * sin_a).astype(BF16)
            dkv_ref[HD:2 * HD, :] = dv[...].T.astype(BF16)


def attn_bwd(scal, qr, d_o, o_t, lse, qkv_t, cos_t, sin_t, qs_row, start, count, carry=None):
    width = count * BQ
    last = carry is not None
    whole = lambda i, s: (0, 0)
    blocked = lambda i, s: (0, i)
    in_specs = [
        pl.BlockSpec((HEADS * HD, BQ), blocked),
        pl.BlockSpec((HEADS * HD, BQ), blocked),
        pl.BlockSpec((HEADS * HD, BQ), blocked),
        pl.BlockSpec((HEADS, BQ), blocked),
        pl.BlockSpec((2 * HD, 2048), lambda i, s: (4, 0)),
        pl.BlockSpec((HALF, 2048), whole),
        pl.BlockSpec((HALF, 2048), whole),
        pl.BlockSpec((1, 2048), whole),
    ]
    scratch = [
        pltpu.VMEM((2048, HD), BF16),
        pltpu.VMEM((HD, 2048), BF16),
        pltpu.VMEM((2048, HD), BF16),
        pltpu.VMEM((HD, HEADS * BQ), BF16),
        pltpu.VMEM((HD, HEADS * BQ), BF16),
        pltpu.VMEM((HEADS, BQ), F32),
        pltpu.VMEM((HD, HEADS * BQ), F32),
        pltpu.VMEM((BK, BQ), F32),
        pltpu.VMEM((BK, HEADS * BQ), BF16),
        pltpu.VMEM((BK, HEADS * BQ), BF16),
    ]
    out_specs = [pl.BlockSpec((HEADS * HD, BQ), blocked)]
    out_shape = [jax.ShapeDtypeStruct((HEADS * HD, width), BF16)]
    args = [scal, qr, d_o, o_t, lse, qkv_t, cos_t, sin_t, qs_row]
    if last:
        in_specs += [pl.BlockSpec((2048, HD), whole)] * 2
        args += list(carry)
        out_specs += [pl.BlockSpec((2 * HD, 2048), whole)]
        out_shape += [jax.ShapeDtypeStruct((2 * HD, 2048), BF16)]
        scratch = [pltpu.VMEM((2048, HD), F32)] * 2 + scratch
    else:
        out_specs += [pl.BlockSpec((2048, HD), whole)] * 2
        out_shape += [jax.ShapeDtypeStruct((2048, HD), F32)] * 2
    return pl.pallas_call(
        functools.partial(attn_bwd_kernel, start, last),
        grid_spec=pltpu.PrefetchScalarGridSpec(
            num_scalar_prefetch=1, grid=(count,), in_specs=in_specs, out_specs=out_specs, scratch_shapes=scratch),
        out_shape=out_shape,
        compiler_params=pltpu.CompilerParams(dimension_semantics=("arbitrary",), vmem_limit_bytes=56 << 20),
        cost_estimate=pl.CostEstimate(flops=int(25e9), bytes_accessed=8 << 20, transcendentals=0),
        name="attn_bwd",
    )(*args)


def embed_grad_kernel(order_ref, ids_ref, starts_ref, a_ref, b_ref, c_ref, d_ref, out_ref, rows):
    i = pl.program_id(0)

    @pl.when(i == 0)
    def _():
        for r, ref in enumerate((a_ref, b_ref, c_ref, d_ref)):
            def widen(t, carry, r=r, ref=ref):
                src = pl.multiple_of(t * 16, 16)
                rows[pl.ds(pl.multiple_of(r * 512 + t * 16, 16), 16), :] = ref[pl.ds(src, 16), :].astype(F32)
                return carry
            lax.fori_loop(0, 32, widen, 0)

    out_ref[...] = jnp.zeros_like(out_ref)
    base = i * ROWS_OUT

    def add_row(t, carry):
        dst = ids_ref[t] - base
        out_ref[pl.ds(dst, 1), :] += rows[pl.ds(order_ref[t], 1), :]
        return carry

    lax.fori_loop(starts_ref[i], starts_ref[i + 1], add_row, 0)


def embed_grad(order, ids, starts, shards, vocab_local):
    blocks = vocab_local // ROWS_OUT
    whole = lambda i, o, d, s: (0, 0)
    return pl.pallas_call(
        embed_grad_kernel,
        grid_spec=pltpu.PrefetchScalarGridSpec(
            num_scalar_prefetch=3,
            grid=(blocks,),
            in_specs=[pl.BlockSpec((512, 2048), whole)] * 4,
            out_specs=pl.BlockSpec((ROWS_OUT, 2048), lambda i, o, d, s: (i, 0)),
            scratch_shapes=[pltpu.VMEM((2048, 2048), F32)],
        ),
        out_shape=jax.ShapeDtypeStruct((vocab_local, 2048), F32),
        compiler_params=pltpu.CompilerParams(dimension_semantics=("arbitrary",), vmem_limit_bytes=56 << 20),
        cost_estimate=pl.CostEstimate(flops=int(30e9), bytes_accessed=75 << 20, transcendentals=0),
        name="embed_grad",
    )(order, ids, starts, *shards)


def solution(mesh):
    def exch(value, bits):
        return lax.ppermute(value, "tp", [(i, i ^ bits) for i in range(4)])

    def gather_shards(value):
        near = exch(value, 1)
        far = exch(value, 2)
        return value, near, far, exch(far, 1)

    def add_f32(*terms):
        total = terms[0].astype(F32)
        for term in terms[1:]:
            total = total + term.astype(F32)
        return total

    def reduce_shards(own, near, far, diag, gate=None):
        far_sum = add_f32(far, exch(diag, 1)).astype(BF16)
        if gate is not None:
            far_sum, _ = lax.optimization_barrier((far_sum, gate))
        return add_f32(own, exch(near, 1), exch(far_sum, 2))

    def all_sum(value):
        value = value + exch(value, 1)
        return value + exch(value, 2)

    def device_step(tokens, doc_ids, embedding, attn_norm, w_q, w_k, w_v, w_o, mlp_norm, w_gate, w_up, w_down, d_out):
        vocab_local, dim = embedding.shape
        me = lax.axis_index("tp")
        tok_abs = tokens.reshape(4, 512)
        local = [tok_abs[me ^ r] - me * vocab_local for r in range(4)]

        def rows_of(r):
            ids = local[r]
            found = jnp.take(embedding, jnp.clip(ids, 0, vocab_local - 1), axis=0)
            return jnp.where(((ids >= 0) & (ids < vocab_local))[:, None], found, jnp.zeros((), BF16))

        part3 = rows_of(3)
        part2 = rows_of(2)
        part1 = rows_of(1)
        part0 = rows_of(0)
        x_emb = reduce_shards(part0, part1, part2, part3).astype(BF16)

        w_qkv = jnp.concatenate([w_q.reshape(dim, HEADS * HD), w_k.reshape(dim, HD), w_v.reshape(dim, HD)], axis=1)
        w_out = w_o.reshape(HEADS * HD, dim)
        positions = jnp.concatenate([(me ^ r) * 512 + jnp.arange(512) for r in range(4)])
        cos_t, sin_t = rope_tables_t(positions)
        docs = doc_ids.reshape(-1)
        doc_start = jnp.sum((docs[:, None] < docs[None, :]).astype(jnp.int32), axis=0)
        start4 = doc_start.reshape(4, 512)
        qs_row = jnp.concatenate([start4[me ^ r] for r in range(4)]).reshape(1, 2048)
        scal = jnp.concatenate([doc_start[::BQ] // BK, me.reshape(1).astype(jnp.int32)])

        keys = jnp.concatenate(local)
        keys = jnp.where((keys >= 0) & (keys < vocab_local), keys, vocab_local)
        sorted_ids, order = lax.sort((keys, jnp.arange(2048, dtype=jnp.int32)), num_keys=1)
        edges = jnp.arange(0, vocab_local + 1, ROWS_OUT, dtype=jnp.int32)
        starts = jnp.sum((sorted_ids[None, :] < edges[:, None]).astype(jnp.int32), axis=1)

        h_one, inv_one = rms_forward(x_emb, attn_norm)
        h_sh = gather_shards(h_one)
        h_near = jnp.concatenate(h_sh[:2])
        h_far = jnp.concatenate(h_sh[2:])
        qkv_t = jnp.concatenate([dot(w_qkv, h_near, 0, 1).astype(BF16), dot(w_qkv, h_far, 0, 1).astype(BF16)], axis=1)

        d_out_late, _ = lax.optimization_barrier((d_out.reshape(512, dim), h_sh[2]))
        do_sh = gather_shards(d_out_late)
        do_near = jnp.concatenate(do_sh[:2])
        do_far = jnp.concatenate(do_sh[2:])

        o_far, qr_far, lse_far = attn_fwd(scal, qkv_t, cos_t, sin_t, qs_row, 4, 4)
        ap_far = dot(o_far, w_out, 0, 0).astype(BF16)
        o_near, qr_near, lse_near = attn_fwd(scal, qkv_t, cos_t, sin_t, qs_row, 0, 4)
        ap_near = dot(o_near, w_out, 0, 0).astype(BF16)
        attn_sum = reduce_shards(ap_near[:512], ap_near[512:], ap_far[:512], ap_far[512:]).astype(BF16)
        x_mid = (x_emb.astype(F32) + attn_sum.astype(F32)).astype(BF16)

        h_two, inv_two = rms_forward(x_mid, mlp_norm)
        h2_sh = gather_shards(h_two)

        def mlp(h_half, do_half):
            gate = dot(h_half, w_gate, 1, 0).astype(BF16)
            up = dot(h_half, w_up, 1, 0).astype(BF16)
            gate32 = gate.astype(F32)
            up32 = up.astype(F32)
            sig = jax.nn.sigmoid(gate32)
            act = gate32 * sig
            mid = (act * up32).astype(BF16)
            d_mid = dot(do_half, w_down, 1, 1)
            d_up = (d_mid * act).astype(BF16)
            d_gate = (d_mid * up32 * sig * (1.0 + gate32 * (1.0 - sig))).astype(BF16)
            d_h = (dot(d_gate, w_gate, 1, 1) + dot(d_up, w_up, 1, 1)).astype(BF16)
            return mid, d_up, d_gate, d_h

        h2_near = jnp.concatenate(h2_sh[:2])
        h2_far = jnp.concatenate(h2_sh[2:])
        mid_near, du_near, dg_near, dh2_near = mlp(h2_near, do_near)
        mid_far, du_far, dg_far, dh2_far = mlp(h2_far, do_far)
        d_h_two = reduce_shards(dh2_near[:512], dh2_near[512:], dh2_far[:512], dh2_far[512:])

        d_mid_norm, d_mlp_norm = rms_backward(d_h_two, x_mid, inv_two, mlp_norm)
        d_x_mid32 = d_out.reshape(512, dim).astype(F32) + d_mid_norm
        dx_sh = gather_shards(d_x_mid32.astype(BF16))
        dx_near = jnp.concatenate(dx_sh[:2])
        dx_far = jnp.concatenate(dx_sh[2:])

        down_near = dot(mid_near, w_down, 1, 0).astype(BF16)
        down_far = dot(mid_far, w_down, 1, 0).astype(BF16)
        y_sum = reduce_shards(down_near[:512], down_near[512:], down_far[:512], down_far[512:], gate=dx_sh[2])
        y_out = (x_mid.astype(F32) + y_sum.astype(BF16).astype(F32)).astype(BF16).reshape(1, 512, dim)

        da_near = dot(w_out, dx_near, 1, 1).astype(BF16)
        da_far = dot(w_out, dx_far, 1, 1).astype(BF16)
        dq_near, dk_acc, dv_acc = attn_bwd(scal, qr_near, da_near, o_near, lse_near, qkv_t, cos_t, sin_t, qs_row, 0, 4)
        dq_far, dkv_t = attn_bwd(scal, qr_far, da_far, o_far, lse_far, qkv_t, cos_t, sin_t, qs_row, 4, 4,
                                 carry=(dk_acc, dv_acc))
        dqkv_far = jnp.concatenate([dq_far, dkv_t[:, 1024:]], axis=0)
        dqkv_near = jnp.concatenate([dq_near, dkv_t[:, :1024]], axis=0)
        dh1_far = dot(dqkv_far, w_qkv, 0, 1).astype(BF16)
        dh1_near = dot(dqkv_near, w_qkv, 0, 1).astype(BF16)
        d_h_one = reduce_shards(dh1_near[:512], dh1_near[512:], dh1_far[:512], dh1_far[512:])

        d_emb_norm, d_attn_norm = rms_backward(d_h_one, x_emb, inv_one, attn_norm)
        dxe_sh = gather_shards((d_x_mid32 + d_emb_norm).astype(BF16))
        d_embedding = embed_grad(order, sorted_ids, starts, dxe_sh, vocab_local)

        mid_all = jnp.concatenate([mid_near, mid_far])
        do_all = jnp.concatenate([do_near, do_far])
        h2_all = jnp.concatenate([h2_near, h2_far])
        d_w_down = dot(mid_all, do_all, 0, 0)
        d_w_gate = dot(h2_all, jnp.concatenate([dg_near, dg_far]), 0, 0)
        d_w_up = dot(h2_all, jnp.concatenate([du_near, du_far]), 0, 0)
        d_w_o = dot(jnp.concatenate([o_near, o_far], axis=1), jnp.concatenate([dx_near, dx_far]), 1, 0)
        d_w_qkv = dot(jnp.concatenate([h_near, h_far]), jnp.concatenate([dqkv_near, dqkv_far], axis=1), 0, 1)
        d_w_q = d_w_qkv[:, :HEADS * HD].reshape(dim, HEADS, HD)
        d_w_k = d_w_qkv[:, HEADS * HD:HEADS * HD + HD].reshape(dim, 1, HD)
        d_w_v = d_w_qkv[:, HEADS * HD + HD:].reshape(dim, 1, HD)
        gains = all_sum(jnp.stack([d_attn_norm, d_mlp_norm]))
        return (y_out, d_embedding, gains[0], d_w_q, d_w_k, d_w_v, d_w_o.reshape(HEADS, HD, dim), gains[1],
                d_w_gate, d_w_up, d_w_down)

    in_specs = (P("dp", None), P("dp", None), P("tp", None), P(None), P(None, "tp", None), P(None, "tp", None),
                P(None, "tp", None), P("tp", None, None), P(None), P(None, "tp"), P(None, "tp"), P("tp", None),
                P("dp", "tp", None))
    out_specs = (P("dp", "tp", None), P(("dp", "tp"), None), P("dp"), P("dp", "tp", None), P("dp", "tp", None),
                 P("dp", "tp", None), P(("dp", "tp"), None, None), P("dp"), P("dp", "tp"), P("dp", "tp"),
                 P(("dp", "tp"), None))
    return jax.shard_map(device_step, mesh=mesh, in_specs=in_specs, out_specs=out_specs, check_vma=False)
```
